32 devices in a mesh: dp: 8 (over z, y), mp: 4 (over x, core).
Axes of the slice: x: 2, y: 2, z: 4, core: 2. Of those that a mesh axis runs over, the one named last changes fastest.
Arguments:
- pixels: bfloat16 [20480, 1280], P(('dp', 'mp')), may hold values from -6 to 6
- embed_weight: bfloat16 [4, 1280, 1024], P(None, None, 'mp'), may hold values from -0.15625 to 0.15625
- embed_bias: bfloat16 [4, 1024], replicated, may hold values from -3 to 3
- first_gain: float32 [1024], replicated, may hold values from 0.5 to 1.5
- first_shift: float32 [1024], replicated, may hold values from -1.75 to 1.75
- query_weight: bfloat16 [1024, 1024], P(None, 'mp'), may hold values from -0.1875 to 0.1875
- query_bias: bfloat16 [1024], P('mp'), may hold values from -1.75 to 1.75
- key_weight: bfloat16 [1024, 1024], P(None, 'mp'), may hold values from -0.1875 to 0.1875
- value_weight: bfloat16 [1024, 1024], P(None, 'mp'), may hold values from -0.1875 to 0.1875
- value_bias: bfloat16 [1024], P('mp'), may hold values from -1.75 to 1.75
- output_weight: bfloat16 [1024, 1024], P('mp'), may hold values from -3 to 3
- output_bias: bfloat16 [1024], replicated, may hold values from -1.75 to 1.75
- second_gain: float32 [1024], replicated, may hold values from 0.5 to 1.5
- second_shift: float32 [1024], replicated, may hold values from -1.75 to 1.75
- up_weight: bfloat16 [1024, 4096], P(None, 'mp'), may hold values from -0.1875 to 0.1875
- up_bias: bfloat16 [4096], P('mp'), may hold values from -1.75 to 1.75
- down_weight: bfloat16 [4096, 1024], P('mp'), may hold values from -0.09375 to 0.09375
- down_bias: bfloat16 [1024], replicated, may hold values from -1.75 to 1.75
- cotangent: bfloat16 [20480, 1024], P(('dp', 'mp')), may hold values from -6 to 6
- item_lengths: int32 [8, 5], P('dp'), may hold values from 1 to 588, 2520 in all within a row
- item_kind: int32 [8, 5], P('dp'), may hold values from 0 to 1
- sampling_level: int32 [8, 5], P('dp'), may hold values from 0 to 7
Outputs:
- layer_output: bfloat16 [20480, 1024], P(('dp', 'mp'))
- pixel_gradient: float32 [20480, 1280], P(('dp', 'mp'))
- embed_weight_gradient: float32 [4, 1280, 1024], P(None, None, 'mp')
- embed_bias_gradient: float32 [4, 1024], replicated
- first_gain_gradient: float32 [1024], replicated
- first_shift_gradient: float32 [1024], replicated
- query_weight_gradient: float32 [1024, 1024], P(None, 'mp')
- query_bias_gradient: float32 [1024], P('mp')
- key_weight_gradient: float32 [1024, 1024], P(None, 'mp')
- value_weight_gradient: float32 [1024, 1024], P(None, 'mp')
- value_bias_gradient: float32 [1024], P('mp')
- output_weight_gradient: float32 [1024, 1024], P('mp')
- output_bias_gradient: float32 [1024], replicated
- second_gain_gradient: float32 [1024], replicated
- second_shift_gradient: float32 [1024], replicated
- up_weight_gradient: float32 [1024, 4096], P(None, 'mp')
- up_bias_gradient: float32 [4096], P('mp')
- down_weight_gradient: float32 [4096, 1024], P('mp')
- down_bias_gradient: float32 [1024], replicated
The draws below stay inside these ranges and needn't reach their ends.
Inputs may be any that keep to these rules, and one draw needn't show every extreme that they name: `item_lengths`: in each group the 5 lengths add up to 2520, the largest is 588; the rows after the items are padding.
All inputs are finite; a program needn't handle non-finite values.
Results may differ from the reference program's by a relative error of at most 0.02.
Values may be sent and summed in bfloat16 or wider, within the bound.
A program may use at most 320 MiB of HBM per device.

```python
import math
import jax
import jax.numpy as jnp
import numpy as np
from jax import lax

D = 1024
HEADS = 16
HD = 64
FF = 4096
PIX = 1280
NG = 4
GRID = 14
NGSD = 8
QB = 512
KW = 2560
ITEM_MAX = 588
TOK_GROUP = 2560
GROUPS = 8
TOKENS = 20480
ITEMS = 5
PAD = 40


def place_ends(values, key, least, high):
    index_at = [jax.random.randint(jax.random.fold_in(key, axis), (), 0, length) for axis, length in enumerate(values.shape)]
    longest = values.shape.index(max(values.shape))
    next_to = index_at[:longest] + [(index_at[longest] + 1) % values.shape[longest]] + index_at[longest + 1:]
    return values.at[tuple(index_at)].set(least).at[tuple(next_to)].set(high)


def steps_of(rng, shape, split, low, largest):
    def one(position, parts):
        heights = jax.random.uniform(jax.random.fold_in(jax.random.fold_in(rng, 6), position), (parts,), jnp.float32, low / len(split), largest / len(split))
        return jnp.repeat(jnp.exp(heights), shape[position] // parts).reshape((-1,) + (1,) * (len(shape) - position - 1))

    level = one(*split[0])
    for cut in split[1:]:
        level = level * one(*cut)
    return level


def length_profile(amount, total, reach, slope):
    loads = [(1 << 20) // math.isqrt(rank ** slope) + 1 for rank in range(2, amount + 1)]
    spare, counts = total - reach - (amount - 1), [1] * (amount - 1)
    while spare > 0:
        free = [i for i in range(amount - 1) if counts[i] < reach]
        whole, left = sum([loads[i] for i in free]), spare
        for i in free:
            more = min(reach - counts[i], max(1, left * loads[i] // whole), spare)
            counts[i] = counts[i] + more
            spare = spare - more
    return np.array([reach] + counts)


def uneven(own_key, number_of, total, limit, slope):
    if number_of == 2:
        one = jax.random.randint(own_key, (), max(1, total - limit), min(limit, total - 1) + 1)
        return jnp.stack([one, total - one])
    tallies = jnp.asarray(length_profile(number_of, total, limit, slope), jnp.int32)
    couples = (number_of - 1) // 2
    source_of, taker = tallies[1:1 + 2 * couples:2], tallies[2:2 + 2 * couples:2]
    room = jnp.minimum(source_of - 1, limit - taker)
    moved = jax.random.randint(jax.random.fold_in(own_key, 1), (couples,), 0, 1 << 20) % (room + 1)
    tallies = tallies.at[1:1 + 2 * couples:2].set(source_of - moved).at[2:2 + 2 * couples:2].set(taker + moved)
    return tallies[jax.random.permutation(jax.random.fold_in(own_key, 2), number_of)]


def normal_values(rng, shape, scale, reach, shards=(), held_as=jnp.bfloat16):
    entries = scale * jax.random.normal(rng, shape, jnp.float32)
    if shards:
        entries = entries * steps_of(rng, shape, shards, -0.22, 0.18)
    return jnp.clip(entries, -reach, reach).astype(held_as)


def setup_inputs(seed: int = 0) -> dict:
    key_of = jax.random.split(jax.random.key(seed), 23)
    return {
        "pixels": normal_values(key_of[0], (TOKENS, PIX), 1.0, 6.0, ((0, 32),)),
        "embed_weight": normal_values(key_of[1], (NG, PIX, D), PIX ** -0.5, 0.15625, ((2, 4),)),
        "embed_bias": normal_values(key_of[2], (NG, D), 0.5, 3.0),
        "first_gain": jnp.clip(1.0 + 0.1 * jax.random.normal(key_of[3], (D,), jnp.float32), 0.5, 1.5),
        "first_shift": normal_values(key_of[4], (D,), 0.3, 1.75, (), jnp.float32),
        "query_weight": normal_values(key_of[5], (D, D), D ** -0.5, 0.1875, ((1, 4),)),
        "query_bias": normal_values(key_of[6], (D,), 0.3, 1.75, ((0, 4),)),
        "key_weight": normal_values(key_of[7], (D, D), D ** -0.5, 0.1875, ((1, 4),)),
        "value_weight": normal_values(key_of[8], (D, D), D ** -0.5, 0.1875, ((1, 4),)),
        "value_bias": normal_values(key_of[9], (D,), 0.3, 1.75, ((0, 4),)),
        "output_weight": normal_values(key_of[10], (D, D), (max(D // 256, 1)) ** -0.5, 3.0, ((0, 4),)),
        "output_bias": normal_values(key_of[11], (D,), 0.3, 1.75),
        "second_gain": jnp.clip(1.0 + 0.1 * jax.random.normal(key_of[12], (D,), jnp.float32), 0.5, 1.5),
        "second_shift": normal_values(key_of[13], (D,), 0.3, 1.75, (), jnp.float32),
        "up_weight": normal_values(key_of[14], (D, FF), D ** -0.5, 0.1875, ((1, 4),)),
        "up_bias": normal_values(key_of[15], (FF,), 0.3, 1.75, ((0, 4),)),
        "down_weight": normal_values(key_of[16], (FF, D), FF ** -0.5, 0.09375, ((0, 4),)),
        "down_bias": normal_values(key_of[17], (D,), 0.3, 1.75),
        "cotangent": normal_values(key_of[18], (TOKENS, D), 1.0, 6.0, ((0, 32),)),
        "item_lengths": jax.vmap(lambda own: uneven(own, ITEMS, TOK_GROUP - PAD, ITEM_MAX, 2))(jax.random.split(key_of[19], GROUPS)).reshape((GROUPS, ITEMS)).astype(jnp.int32),
        "item_kind": place_ends(jax.random.randint(key_of[20], (GROUPS, ITEMS), 0, 2), jax.random.fold_in(key_of[20], 1), 0, 1).astype(jnp.int32),
        "sampling_level": place_ends(jax.random.randint(key_of[21], (GROUPS, ITEMS), 0, NGSD), jax.random.fold_in(key_of[21], 1), 0, NGSD - 1).astype(jnp.int32),
    }


@jax.custom_vjp
def low(v):
    return lax.optimization_barrier(v.astype(jnp.bfloat16)).astype(jnp.float32)

@jax.custom_vjp
def low_back(v):
    return v

def low_keep(v):
    return (low(v), None)

def low_pass(kept, grad):
    return (grad,)

def back_keep(v):
    return (v, None)

def back_low(kept, grad):
    return (low(grad),)
low.defvjp(low_keep, low_pass)
low_back.defvjp(back_keep, back_low)
HIGHEST_PRECISION = lax.Precision.HIGHEST

def matmul(left, right):
    return jnp.dot(left, right, precision=HIGHEST_PRECISION, preferred_element_type=jnp.float32)

def both_ways(value):
    return low_back(low(value))

def row_tables(lengths, kinds, levels, row_number, used_rows, grid_side):
    ends = jnp.cumsum(lengths, dtype=jnp.int32)
    starts = (ends - lengths).astype(jnp.int32)
    segment = lax.optimization_barrier(jnp.sum((row_number[:, None] >= ends[None, :]).astype(jnp.int32), axis=1, dtype=jnp.int32))
    starts_all = jnp.concatenate([starts, jnp.full((1,), used_rows, jnp.int32)])
    kinds_all = jnp.concatenate([kinds.astype(jnp.int32), jnp.ones((1,), jnp.int32)])
    levels_all = jnp.concatenate([levels.astype(jnp.int32), jnp.zeros((1,), jnp.int32)])
    selector = segment[:, None] == jnp.arange(lengths.shape[0] + 1, dtype=jnp.int32)[None, :]
    row_begin = lax.optimization_barrier(jnp.sum(jnp.where(selector, starts_all[None, :], 0), axis=1, dtype=jnp.int32))
    row_kind = lax.optimization_barrier(jnp.sum(jnp.where(selector, kinds_all[None, :], 0), axis=1, dtype=jnp.int32))
    row_level = lax.optimization_barrier(jnp.sum(jnp.where(selector, levels_all[None, :], 0), axis=1, dtype=jnp.int32))
    offset = (row_number - row_begin).astype(jnp.int32)
    band = jnp.where(row_kind == 0, offset // (grid_side * grid_side) % 3, 3).astype(jnp.int32)
    return (segment, offset, band, row_level)

def position_code(offset, level, model_width, grid_side):
    quarter = model_width // 4
    cell = offset % (grid_side * grid_side)
    row_place = (cell // grid_side).astype(jnp.float32)
    col_place = (cell % grid_side).astype(jnp.float32)
    scale = jnp.exp2(level.astype(jnp.float32) * 0.5 - 1.5)
    freq = jnp.exp(jnp.arange(quarter).astype(jnp.float32) * (-math.log(10000.0) / quarter))
    row_angle = (row_place * scale)[:, None] * freq[None, :]
    col_angle = (col_place * scale)[:, None] * freq[None, :]
    return jnp.concatenate([jnp.sin(row_angle), jnp.cos(row_angle), jnp.sin(col_angle), jnp.cos(col_angle)], axis=1)

def layer_norm(values, gain, shift):
    center = lax.optimization_barrier(jnp.mean(values, axis=-1, keepdims=True))
    centered = values - center
    spread = lax.optimization_barrier(jnp.mean(centered * centered, axis=-1, keepdims=True))
    return centered * lax.rsqrt(spread + 1e-06) * gain + shift

def attend(query, keys, values, segment):
    total_rows = query.shape[0]

    def one_block(block_index):
        query_start = block_index * QB
        key_start = jnp.clip(query_start - 2 * QB, 0, total_rows - KW)
        query_block = lax.dynamic_slice_in_dim(query, query_start, QB, 0)
        key_block = lax.dynamic_slice_in_dim(keys, key_start, KW, 0)
        value_block = lax.dynamic_slice_in_dim(values, key_start, KW, 0)
        query_segment = lax.dynamic_slice_in_dim(segment, query_start, QB, 0)
        key_segment = lax.dynamic_slice_in_dim(segment, key_start, KW, 0)
        allowed = (query_segment[:, None] == key_segment[None, :])[None]
        scores = low_back(jnp.einsum('qhd,khd->hqk', query_block, key_block, precision=HIGHEST_PRECISION) * 0.125)
        scores = jnp.where(allowed, scores, -1e+30)
        highest = lax.optimization_barrier(jnp.max(scores, axis=2, keepdims=True))
        weights = jnp.exp(scores - highest)
        softmax_rows = weights / lax.optimization_barrier(jnp.sum(weights, axis=2, keepdims=True))
        return jnp.einsum('hqk,khd->qhd', low(softmax_rows), value_block, precision=HIGHEST_PRECISION)
    blocks = lax.map(jax.checkpoint(one_block), jnp.arange(total_rows // QB, dtype=jnp.int32))
    return blocks.reshape(query.shape)

def layer_forward(params, pixel_values, band_hot, code, segment):
    embed_weight, embed_bias, first_gain, first_shift, query_weight, query_bias, key_weight, value_weight, value_bias, output_weight, output_bias, second_gain, second_shift, up_weight, up_bias, down_weight, down_bias = params
    total_rows = pixel_values.shape[0]
    expanded = (band_hot[:, :, None] * pixel_values[:, None, :]).reshape(total_rows, NG * PIX)
    embedded = low_back(matmul(expanded, embed_weight.reshape(NG * PIX, D)))
    start = embedded + matmul(band_hot, embed_bias) + code
    normed1 = low(layer_norm(start, first_gain, first_shift))
    query = both_ways(matmul(normed1, query_weight) + query_bias)
    keys = both_ways(matmul(normed1, key_weight))
    values = both_ways(matmul(normed1, value_weight) + value_bias)
    shaped = (total_rows, HEADS, HD)
    attended = attend(query.reshape(shaped), keys.reshape(shaped), values.reshape(shaped), segment)
    mixed = both_ways(attended.reshape(total_rows, D))
    middle = start + low_back(matmul(mixed, output_weight)) + output_bias
    normed2 = low(layer_norm(middle, second_gain, second_shift))
    hidden = low_back(matmul(normed2, up_weight) + up_bias)
    activated = low(jax.nn.gelu(hidden, approximate=False))
    return middle + low_back(matmul(activated, down_weight)) + down_bias

def add_trees(left, right):
    return jax.tree.map(jnp.add, left, right)

def reference(pixels, embed_weight, embed_bias, first_gain, first_shift, query_weight, query_bias, key_weight, value_weight, value_bias, output_weight, output_bias, second_gain, second_shift, up_weight, up_bias, down_weight, down_bias, cotangent, item_lengths, item_kind, sampling_level):
    params = tuple((item.astype(jnp.float32) for item in (embed_weight, embed_bias, first_gain, first_shift, query_weight, query_bias, key_weight, value_weight, value_bias, output_weight, output_bias, second_gain, second_shift, up_weight, up_bias, down_weight, down_bias)))
    used_rows = TOK_GROUP - PAD
    row_number = jnp.arange(TOK_GROUP, dtype=jnp.int32)
    valid = (row_number < used_rows).astype(jnp.float32)[:, None]

    def group_step(totals, inputs):
        pixel_rows, cot_rows, lengths, kinds, levels = inputs
        segment, offset, band, level = row_tables(lengths, kinds, levels, row_number, used_rows, GRID)
        band_hot = (band[:, None] == jnp.arange(NG, dtype=jnp.int32)[None, :]).astype(jnp.float32)
        code = position_code(offset, level, D, GRID)

        def forward(weights, pixel_values):
            return layer_forward(weights, pixel_values, band_hot, code, segment)
        final, pullback = jax.vjp(forward, params, pixel_rows.astype(jnp.float32))
        weight_grads, pixel_grads = pullback(cot_rows.astype(jnp.float32) * valid)
        return (add_trees(totals, weight_grads), (final.astype(jnp.bfloat16), pixel_grads))
    zeros = jax.tree.map(jnp.zeros_like, params)
    inputs = (pixels.reshape(GROUPS, TOK_GROUP, PIX), cotangent.reshape(GROUPS, TOK_GROUP, D), item_lengths, item_kind, sampling_level)
    totals, (outputs, pixel_grads) = lax.scan(group_step, zeros, inputs)
    return (outputs.reshape(TOKENS, D), pixel_grads.reshape(TOKENS, PIX), totals[0], totals[1], totals[2], totals[3], totals[4], totals[5], totals[6], totals[7], totals[8], totals[9], totals[10], totals[11], totals[12], totals[13], totals[14], totals[15], totals[16])
```

```python
import math

import jax
import jax.numpy as jnp
from jax import lax
from jax.experimental import pallas as pl
from jax.experimental.pallas import tpu as pltpu
from jax.sharding import PartitionSpec as P

HD = 64
GRID = 14
ITEM_MAX = 588
ALIGN = 16
CHUNK = 128
WINDOW = 640
SCORE_SCALE = 0.125 * math.log2(math.e)


HIGHEST_PRECISION = lax.Precision.HIGHEST
INV_ROOT_TWO = 1.0 / math.sqrt(2.0)
INV_ROOT_TAU = 1.0 / math.sqrt(2.0 * math.pi)


def row_tables(lengths, kinds, levels, row_number, used_rows, grid_side):
    ends = jnp.cumsum(lengths, dtype=jnp.int32)
    starts = ends - lengths
    segment = jnp.sum(
        (row_number[:, None] >= ends[None, :]).astype(jnp.int32), axis=1, dtype=jnp.int32
    )
    starts_all = jnp.concatenate([starts, jnp.full((1,), used_rows, jnp.int32)])
    kinds_all = jnp.concatenate([kinds, jnp.ones((1,), jnp.int32)])
    levels_all = jnp.concatenate([levels, jnp.zeros((1,), jnp.int32)])
    selector = segment[:, None] == jnp.arange(lengths.shape[0] + 1, dtype=jnp.int32)[None, :]
    row_begin = jnp.sum(jnp.where(selector, starts_all[None, :], 0), axis=1, dtype=jnp.int32)
    row_kind = jnp.sum(jnp.where(selector, kinds_all[None, :], 0), axis=1, dtype=jnp.int32)
    row_level = jnp.sum(jnp.where(selector, levels_all[None, :], 0), axis=1, dtype=jnp.int32)
    offset = row_number - row_begin
    band = jnp.where(row_kind == 0, offset // (grid_side * grid_side) % 3, 3)
    return (segment, offset, band, row_level)


def position_code(offset, level, model_width, grid_side):
    quarter = model_width // 4
    cell = offset % (grid_side * grid_side)
    row_place = (cell // grid_side).astype(jnp.float32)
    col_place = (cell % grid_side).astype(jnp.float32)
    scale = jnp.exp2(level.astype(jnp.float32) * 0.5 - 1.5)
    freq = jnp.exp(jnp.arange(quarter).astype(jnp.float32) * (-math.log(10000.0) / quarter))
    row_angle = (row_place * scale)[:, None] * freq[None, :]
    col_angle = (col_place * scale)[:, None] * freq[None, :]
    return jnp.concatenate(
        [jnp.sin(row_angle), jnp.cos(row_angle), jnp.sin(col_angle), jnp.cos(col_angle)], axis=1
    )


def norm_parts(values, gain, shift):
    center = jnp.mean(values, axis=-1, keepdims=True)
    centered = values - center
    spread = jnp.mean(centered * centered, axis=-1, keepdims=True)
    inverse = lax.rsqrt(spread + 1e-06)
    scaled = centered * inverse
    return ((scaled * gain + shift).astype(jnp.bfloat16), scaled, inverse)


def norm_back(grad_rows, scaled, inverse, gain):
    weighted = grad_rows * gain
    return inverse * (
        weighted
        - jnp.mean(weighted, axis=-1, keepdims=True)
        - scaled * jnp.mean(weighted * scaled, axis=-1, keepdims=True)
    )


def gelu_slope(hidden):
    return (
        0.5 * (1.0 + lax.erf(hidden * INV_ROOT_TWO))
        + hidden * jnp.exp(-0.5 * hidden * hidden) * INV_ROOT_TAU
    )


def item_table(lengths, used_rows, total_rows):
    ends = jnp.cumsum(lengths, dtype=jnp.int32)
    starts = jnp.concatenate([ends - lengths, jnp.full((1,), used_rows, jnp.int32)])
    ends = jnp.concatenate([ends, jnp.full((1,), total_rows, jnp.int32)])
    begin = jnp.minimum(starts // ALIGN * ALIGN, total_rows - WINDOW)
    low = starts - begin
    high = ends - begin
    return jnp.stack([begin, low, high, (high + CHUNK - 1) // CHUNK])


def head_masks():
    lane = lax.broadcasted_iota(jnp.int32, (1, 2 * HD), 1)
    first = lane < HD
    return first, first.astype(jnp.bfloat16), (lane >= HD).astype(jnp.bfloat16)


def two_heads(block, mask_a, mask_b):
    return jnp.concatenate([block * mask_a, block * mask_b], axis=0)


def product(left, right, left_dim, right_dim):
    return lax.dot_general(
        left,
        right,
        (((left_dim,), (right_dim,)), ((), ())),
        preferred_element_type=jnp.float32,
    )


def forward_kernel(table, qkv_ref, out_ref, stat_ref):
    first, mask_a, mask_b = head_masks()
    pair = 2 * HD

    def one_item(item, carry):
        begin = pl.multiple_of(table[0, item], ALIGN)
        low = table[1, item]
        high = table[2, item]
        keys = qkv_ref[pl.ds(begin, WINDOW), pair : 2 * pair]
        values = qkv_ref[pl.ds(begin, WINDOW), 2 * pair : 3 * pair]
        extended = jnp.concatenate([values, jnp.ones((WINDOW, pair), jnp.bfloat16)], axis=1)
        place = lax.broadcasted_iota(jnp.int32, (1, WINDOW), 1)
        bias = jnp.where((place >= low) & (place < high), 0.0, -1e30)

        def one_chunk(chunk, inner):
            rows = pl.ds(pl.multiple_of(begin + chunk * CHUNK, ALIGN), CHUNK)
            stacked = two_heads(qkv_ref[rows, 0:pair], mask_a, mask_b)
            scores = product(stacked, keys, 1, 1) * SCORE_SCALE + bias
            highest = jnp.max(scores, axis=1, keepdims=True)
            weights = jnp.exp2(scores - highest).astype(jnp.bfloat16)
            sums = product(weights, extended, 1, 0)
            mixed = jnp.where(first, sums[:CHUNK, :pair], sums[CHUNK:, :pair])
            totals = jnp.where(first, sums[:CHUNK, pair:], sums[CHUNK:, pair:])
            tops = jnp.where(first, highest[:CHUNK], highest[CHUNK:])
            row = chunk * CHUNK + lax.broadcasted_iota(jnp.int32, (CHUNK, 1), 0)
            keep = (row >= low) & (row < high)
            out_ref[rows, :] = jnp.where(
                keep, mixed / totals, out_ref[rows, :].astype(jnp.float32)
            ).astype(jnp.bfloat16)
            stat_ref[rows, :] = jnp.where(keep, tops + jnp.log2(totals), stat_ref[rows, :])
            return inner

        lax.fori_loop(0, table[3, item], one_chunk, 0)
        return carry

    lax.fori_loop(0, table.shape[1], one_item, 0)


def backward_kernel(table, qkv_ref, grad_ref, stat_ref, out_ref, key_acc, value_acc):
    first, mask_a, mask_b = head_masks()
    pair = 2 * HD

    def one_item(item, carry):
        begin = pl.multiple_of(table[0, item], ALIGN)
        low = table[1, item]
        high = table[2, item]
        window = pl.ds(begin, WINDOW)
        keys = qkv_ref[window, pair : 2 * pair]
        values = qkv_ref[window, 2 * pair : 3 * pair]
        place = lax.broadcasted_iota(jnp.int32, (WINDOW, 1), 0)
        inside = (place >= low) & (place < high)
        bias = jnp.where(inside, 0.0, -1e30)
        key_acc[...] = jnp.zeros_like(key_acc)
        value_acc[...] = jnp.zeros_like(value_acc)

        def one_chunk(chunk, inner):
            rows = pl.ds(pl.multiple_of(begin + chunk * CHUNK, ALIGN), CHUNK)
            query = two_heads(qkv_ref[rows, 0:pair], mask_a, mask_b)
            grads = two_heads(grad_ref[rows, :], mask_a, mask_b)
            turned = stat_ref[rows, :].T
            stat = jnp.concatenate([turned[0:1], turned[HD : HD + 1]], axis=1)
            spot = lax.broadcasted_iota(jnp.int32, (1, CHUNK), 1) + chunk * CHUNK
            usable = (spot >= low) & (spot < high)
            usable = jnp.concatenate([usable, usable], axis=1)
            stat = jnp.where(usable, stat, 1e30)
            probs = jnp.exp2(product(keys, query, 1, 1) * SCORE_SCALE + bias - stat)
            slope = product(values, grads, 1, 1)
            dots = jnp.sum(probs * slope, axis=0, keepdims=True)
            score_grad = (probs * (slope - dots)).astype(jnp.bfloat16)
            value_acc[...] += product(probs.astype(jnp.bfloat16), grads, 1, 0)
            key_acc[...] += product(score_grad, query, 1, 0)
            query_grad = product(score_grad, keys, 0, 0)
            query_grad = jnp.where(first, query_grad[:CHUNK], query_grad[CHUNK:]) * 0.125
            row = chunk * CHUNK + lax.broadcasted_iota(jnp.int32, (CHUNK, 1), 0)
            keep = (row >= low) & (row < high)
            out_ref[rows, 0:pair] = jnp.where(
                keep, query_grad, out_ref[rows, 0:pair].astype(jnp.float32)
            ).astype(jnp.bfloat16)
            return inner

        lax.fori_loop(0, table[3, item], one_chunk, 0)
        for acc, spot, factor in ((key_acc, 1, 0.125), (value_acc, 2, 1.0)):
            columns = slice(spot * pair, (spot + 1) * pair)
            out_ref[window, columns] = jnp.where(
                inside, acc[...] * factor, out_ref[window, columns].astype(jnp.float32)
            ).astype(jnp.bfloat16)
        return carry

    lax.fori_loop(0, table.shape[1], one_item, 0)


def attention_forward(projected, table):
    total_rows, width = projected.shape
    pair = 2 * HD
    blocks = width // (3 * pair)
    return pl.pallas_call(
        forward_kernel,
        out_shape=(
            jax.ShapeDtypeStruct((total_rows, blocks * pair), jnp.bfloat16),
            jax.ShapeDtypeStruct((total_rows, blocks * pair), jnp.float32),
        ),
        grid_spec=pltpu.PrefetchScalarGridSpec(
            num_scalar_prefetch=1,
            grid=(blocks,),
            in_specs=[pl.BlockSpec((total_rows, 3 * pair), lambda h, _: (0, h))],
            out_specs=(
                pl.BlockSpec((total_rows, pair), lambda h, _: (0, h)),
                pl.BlockSpec((total_rows, pair), lambda h, _: (0, h)),
            ),
        ),
        cost_estimate=pl.CostEstimate(
            flops=blocks * total_rows * WINDOW * 1024,
            bytes_accessed=total_rows * width * 4,
            transcendentals=blocks * total_rows * WINDOW * 2,
        ),
        name="attention_forward",
    )(table, projected)


def attention_backward(projected, mixed_grad, stat, table):
    total_rows, width = projected.shape
    pair = 2 * HD
    blocks = width // (3 * pair)
    return pl.pallas_call(
        backward_kernel,
        out_shape=jax.ShapeDtypeStruct((total_rows, width), jnp.bfloat16),
        grid_spec=pltpu.PrefetchScalarGridSpec(
            num_scalar_prefetch=1,
            grid=(blocks,),
            in_specs=[
                pl.BlockSpec((total_rows, 3 * pair), lambda h, _: (0, h)),
                pl.BlockSpec((total_rows, pair), lambda h, _: (0, h)),
                pl.BlockSpec((total_rows, pair), lambda h, _: (0, h)),
            ],
            out_specs=pl.BlockSpec((total_rows, 3 * pair), lambda h, _: (0, h)),
            scratch_shapes=[
                pltpu.VMEM((WINDOW, pair), jnp.float32),
                pltpu.VMEM((WINDOW, pair), jnp.float32),
            ],
        ),
        cost_estimate=pl.CostEstimate(
            flops=blocks * total_rows * WINDOW * 2560,
            bytes_accessed=total_rows * width * 6,
            transcendentals=blocks * total_rows * WINDOW * 2,
        ),
        name="attention_backward",
    )(table, projected, mixed_grad, stat)


def widen(part):
    extra = -part.shape[-1] % (2 * HD)
    return jnp.pad(part, [(0, 0)] * (part.ndim - 1) + [(0, extra)]) if extra else part


def interleave(query_part, key_part, value_part):
    pair = 2 * HD
    query_part, key_part, value_part = widen(query_part), widen(key_part), widen(value_part)
    lead = query_part.shape[:-1]
    parts = [part.reshape(*lead, -1, 1, pair) for part in (query_part, key_part, value_part)]
    return jnp.concatenate(parts, axis=-2).reshape(*lead, -1)


def separate(merged, width):
    pair = 2 * HD
    lead = merged.shape[:-1]
    split = merged.reshape(*lead, -1, 3, pair)
    return [split[..., spot, :].reshape(*lead, -1)[..., :width] for spot in range(3)]


def per_device(
    pixels,
    embed_weight,
    embed_bias,
    first_gain,
    first_shift,
    query_weight,
    query_bias,
    key_weight,
    value_weight,
    value_bias,
    output_weight,
    output_bias,
    second_gain,
    second_shift,
    up_weight,
    up_bias,
    down_weight,
    down_bias,
    cotangent,
    item_lengths,
    item_kind,
    sampling_level,
):
    tensor_size = lax.axis_size("mp")
    local_rows = pixels.shape[0]
    model_width = embed_bias.shape[1]
    group_rows = local_rows * tensor_size
    used_rows = group_rows - min(group_rows // 64, ITEM_MAX)
    local_width = query_weight.shape[1]
    row_start = lax.axis_index("mp") * local_rows
    all_rows = jnp.arange(group_rows, dtype=jnp.int32)
    segment, offset_all, band_all, level_all = row_tables(
        item_lengths[0], item_kind[0], sampling_level[0], all_rows, used_rows, GRID
    )
    offset = lax.dynamic_slice_in_dim(offset_all, row_start, local_rows, 0)
    band = lax.dynamic_slice_in_dim(band_all, row_start, local_rows, 0)
    level = lax.dynamic_slice_in_dim(level_all, row_start, local_rows, 0)
    band_hot = (band[:, None] == jnp.arange(embed_bias.shape[0], dtype=jnp.int32)[None, :]).astype(
        jnp.float32
    )
    code = position_code(offset, level, model_width, GRID)
    full_embed = lax.all_gather(embed_weight, "mp", axis=2, tiled=True)
    flat_embed = full_embed.reshape(-1, model_width)
    expanded = (band_hot.astype(jnp.bfloat16)[:, :, None] * pixels[:, None, :]).reshape(
        local_rows, -1
    )
    embedded = jnp.dot(expanded, flat_embed, preferred_element_type=jnp.float32)
    start = (
        embedded
        + jnp.dot(band_hot, embed_bias.astype(jnp.float32), precision=HIGHEST_PRECISION)
        + code
    )
    normed1, scaled1, inverse1 = norm_parts(start, first_gain, first_shift)
    gathered1 = lax.all_gather(normed1, "mp", axis=0, tiled=True)
    merged_weight = interleave(query_weight, key_weight, value_weight)
    merged_bias = interleave(
        query_bias.astype(jnp.float32),
        jnp.zeros((local_width,), jnp.float32),
        value_bias.astype(jnp.float32),
    )
    projected = (
        jnp.dot(gathered1, merged_weight, preferred_element_type=jnp.float32) + merged_bias
    ).astype(jnp.bfloat16)
    table = item_table(item_lengths[0], used_rows, group_rows)
    attended, stat = attention_forward(projected, table)
    attended = attended[:, :local_width]
    rows = attended
    branch = lax.psum_scatter(
        jnp.dot(rows, output_weight, preferred_element_type=jnp.float32).astype(jnp.bfloat16),
        "mp",
        scatter_dimension=0,
        tiled=True,
    ).astype(jnp.float32)
    middle = start + branch + output_bias
    normed2, scaled2, inverse2 = norm_parts(middle, second_gain, second_shift)
    gathered2 = lax.all_gather(normed2, "mp", axis=0, tiled=True)
    hidden = jnp.dot(gathered2, up_weight, preferred_element_type=jnp.float32) + up_bias
    activated = jax.nn.gelu(hidden, approximate=False).astype(jnp.bfloat16)
    rows = activated
    mlp_branch = lax.psum_scatter(
        jnp.dot(rows, down_weight, preferred_element_type=jnp.float32).astype(jnp.bfloat16),
        "mp",
        scatter_dimension=0,
        tiled=True,
    ).astype(jnp.float32)
    final = middle + mlp_branch + down_bias
    layer_output = final.astype(jnp.bfloat16)
    own_rows = row_start + jnp.arange(local_rows, dtype=jnp.int32)
    valid = (own_rows < used_rows).astype(jnp.float32)[:, None]
    upstream = cotangent.astype(jnp.float32) * valid
    down_bias_grad = jnp.sum(upstream, axis=0)
    upstream_low = upstream.astype(jnp.bfloat16)
    gathered_grad = lax.all_gather(upstream_low, "mp", axis=0, tiled=True)
    down_weight_grad = jnp.dot(activated.T, gathered_grad, preferred_element_type=jnp.float32)
    hidden_grad = (
        jnp.dot(gathered_grad, down_weight.T, preferred_element_type=jnp.float32)
        * gelu_slope(hidden)
    ).astype(jnp.bfloat16)
    up_bias_grad = jnp.sum(hidden_grad, axis=0, dtype=jnp.float32)
    up_weight_grad = jnp.dot(gathered2.T, hidden_grad, preferred_element_type=jnp.float32)
    rows = hidden_grad
    normed2_grad = lax.psum_scatter(
        jnp.dot(rows, up_weight.T, preferred_element_type=jnp.float32).astype(jnp.bfloat16),
        "mp",
        scatter_dimension=0,
        tiled=True,
    ).astype(jnp.float32)
    second_gain_grad = jnp.sum(normed2_grad * scaled2, axis=0)
    second_shift_grad = jnp.sum(normed2_grad, axis=0)
    middle_grad = upstream + norm_back(normed2_grad, scaled2, inverse2, second_gain)
    output_bias_grad = jnp.sum(middle_grad, axis=0)
    middle_low = middle_grad.astype(jnp.bfloat16)
    gathered_middle = lax.all_gather(middle_low, "mp", axis=0, tiled=True)
    output_weight_grad = jnp.dot(attended.T, gathered_middle, preferred_element_type=jnp.float32)
    mixed_grad = jnp.dot(
        gathered_middle, output_weight.T, preferred_element_type=jnp.float32
    ).astype(jnp.bfloat16)
    merged_grad = attention_backward(projected, widen(mixed_grad), stat, table)
    merged_bias_grad = jnp.sum(merged_grad, axis=0, dtype=jnp.float32)
    query_bias_grad, _, value_bias_grad = separate(merged_bias_grad, local_width)
    merged_weight_grad = jnp.dot(gathered1.T, merged_grad, preferred_element_type=jnp.float32)
    query_weight_part, key_weight_part, value_weight_part = separate(merged_weight_grad, local_width)
    rows = merged_grad
    normed1_grad = lax.psum_scatter(
        jnp.dot(rows, merged_weight.T, preferred_element_type=jnp.float32).astype(jnp.bfloat16),
        "mp",
        scatter_dimension=0,
        tiled=True,
    ).astype(jnp.float32)
    first_gain_grad = jnp.sum(normed1_grad * scaled1, axis=0)
    first_shift_grad = jnp.sum(normed1_grad, axis=0)
    start_grad = middle_grad + norm_back(normed1_grad, scaled1, inverse1, first_gain)
    start_low = start_grad.astype(jnp.bfloat16)
    spread_grad = jnp.dot(start_low, flat_embed.T, preferred_element_type=jnp.float32)
    pixel_gradient = jnp.sum(
        spread_grad.reshape(local_rows, band_hot.shape[1], -1) * band_hot[:, :, None], axis=1
    )
    embed_term = jnp.dot(expanded.T, start_low, preferred_element_type=jnp.float32).reshape(
        full_embed.shape
    )
    embed_weight_grad = lax.psum_scatter(
        embed_term.astype(jnp.bfloat16), "mp", scatter_dimension=2, tiled=True
    )
    embed_bias_grad = jnp.dot(band_hot.T, start_grad, precision=HIGHEST_PRECISION)
    (
        embed_weight_sum,
        query_weight_sum,
        query_bias_sum,
        key_weight_sum,
        value_weight_sum,
        value_bias_sum,
        output_weight_sum,
        up_weight_sum,
        up_bias_sum,
        down_weight_sum,
    ) = (
        lax.psum(embed_weight_grad, "dp").astype(jnp.float32),
        lax.psum(query_weight_part.astype(jnp.bfloat16), "dp").astype(jnp.float32),
        lax.psum(query_bias_grad.astype(jnp.bfloat16), "dp").astype(jnp.float32),
        lax.psum(key_weight_part.astype(jnp.bfloat16), "dp").astype(jnp.float32),
        lax.psum(value_weight_part.astype(jnp.bfloat16), "dp").astype(jnp.float32),
        lax.psum(value_bias_grad.astype(jnp.bfloat16), "dp").astype(jnp.float32),
        lax.psum(output_weight_grad.astype(jnp.bfloat16), "dp").astype(jnp.float32),
        lax.psum(up_weight_grad.astype(jnp.bfloat16), "dp").astype(jnp.float32),
        lax.psum(up_bias_grad.astype(jnp.bfloat16), "dp").astype(jnp.float32),
        lax.psum(down_weight_grad.astype(jnp.bfloat16), "dp").astype(jnp.float32),
    )
    (
        embed_bias_sum,
        first_gain_sum,
        first_shift_sum,
        output_bias_sum,
        second_gain_sum,
        second_shift_sum,
        down_bias_sum,
    ) = lax.psum(
        (
            embed_bias_grad,
            first_gain_grad,
            first_shift_grad,
            output_bias_grad,
            second_gain_grad,
            second_shift_grad,
            down_bias_grad,
        ),
        ("dp", "mp"),
    )
    return (
        layer_output,
        pixel_gradient,
        embed_weight_sum,
        embed_bias_sum,
        first_gain_sum,
        first_shift_sum,
        query_weight_sum,
        query_bias_sum,
        key_weight_sum,
        value_weight_sum,
        value_bias_sum,
        output_weight_sum,
        output_bias_sum,
        second_gain_sum,
        second_shift_sum,
        up_weight_sum,
        up_bias_sum,
        down_weight_sum,
        down_bias_sum,
    )


def solution(mesh):
    placed = (
        P(("dp", "mp"), None),
        P(None, None, "mp"),
        P(),
        P(),
        P(),
        P(None, "mp"),
        P("mp"),
        P(None, "mp"),
        P(None, "mp"),
        P("mp"),
        P("mp", None),
        P(),
        P(),
        P(),
        P(None, "mp"),
        P("mp"),
        P("mp", None),
        P(),
        P(("dp", "mp"), None),
        P("dp", None),
        P("dp", None),
        P("dp", None),
    )
    return jax.shard_map(
        per_device,
        mesh=mesh,
        in_specs=placed,
        out_specs=(
            P(("dp", "mp"), None),
            P(("dp", "mp"), None),
            P(None, None, "mp"),
            P(),
            P(),
            P(),
            P(None, "mp"),
            P("mp"),
            P(None, "mp"),
            P(None, "mp"),
            P("mp"),
            P("mp", None),
            P(),
            P(),
            P(),
            P(None, "mp"),
            P("mp"),
            P("mp", None),
            P(),
        ),
        check_vma=False,
    )
```
